32 devices in a mesh: gx: 16 (over z, y, core), gy: 2 (over x).
Axes of the slice: x: 2, y: 2, z: 4, core: 2. Of those that a mesh axis runs over, the one named last changes fastest.
Arguments:
- populations: float32 [19, 64, 16, 128], P(None, 'gx', 'gy'), may hold values from 0.02 to 0.1
- fluid: int32 [64, 16, 128], P('gx', 'gy'), may hold values 0 or 1
Outputs:
- advanced: float32 [19, 64, 16, 128], P(None, 'gx', 'gy')
The draws below stay inside these ranges and needn't reach their ends.
Inputs may be any that keep to these rules, and one draw needn't show every extreme that they name: 1 marks a fluid cell, 0 a solid one.
All inputs are finite; a program needn't handle non-finite values. No bound on the sum of `fluid` on one device may be relied on, other than what follows from the above.
Results may differ from the reference program's by a relative error of at most 0.0001.
Values sent between devices are 32-bit elements; how exact they have to be, the bound alone decides.
A program may use at most 64 MiB of HBM per device.

```python
import jax
import jax.numpy as jnp
import numpy as np
from jax import lax

NZ = 128
STEPS = 4
NX = 64
NY = 16


def with_ends(values, rng, least, high):
    place = [jax.random.randint(jax.random.fold_in(rng, axis), (), 0, length) for axis, length in enumerate(values.shape)]
    longest = values.shape.index(max(values.shape))
    beside = place[:longest] + [(place[longest] + 1) % values.shape[longest]] + place[longest + 1:]
    return values.at[tuple(place)].set(least).at[tuple(beside)].set(high)


def level_of(own_key, dims, pieces, low, largest):
    loudness = 1.0
    for axis_at, parts in pieces:
        steps = jax.random.uniform(jax.random.fold_in(jax.random.fold_in(own_key, 6), axis_at), (parts,), jnp.float32, low / len(pieces), largest / len(pieces))
        loudness = loudness * jnp.repeat(jnp.exp(steps), dims[axis_at] // parts).reshape((-1,) + (1,) * (len(dims) - 1 - axis_at))
    return loudness


def setup_inputs(seed: int = 0) -> dict:
    keys = jax.random.split(jax.random.key(seed), 3)
    populations = jnp.clip(0.02 + 0.08 * jax.random.uniform(keys[0], (19, NX, NY, NZ), jnp.float32) ** level_of(keys[0], (19, NX, NY, NZ), ((1, 16), (2, 2)), -0.2, 0.2), 0.02, 0.1)
    fluid = with_ends((jax.random.randint(keys[1], (NX, NY, NZ), 0, 8) < 7).astype(jnp.int32), jax.random.fold_in(keys[1], 1), 0, 1)
    return {"populations": populations, "fluid": fluid}


VELOCITIES = np.array([[0, 0, 0], [1, 0, 0], [-1, 0, 0], [0, 1, 0], [0, -1, 0], [0, 0, 1], [0, 0, -1], [1, 1, 0], [-1, -1, 0], [1, -1, 0], [-1, 1, 0], [1, 0, 1], [-1, 0, -1], [1, 0, -1], [-1, 0, 1], [0, 1, 1], [0, -1, -1], [0, 1, -1], [0, -1, 1]])
OPPOSITE = [0, 2, 1, 4, 3, 6, 5, 8, 7, 10, 9, 12, 11, 14, 13, 16, 15, 18, 17]
WEIGHTS = [1.0 / 3.0] + [1.0 / 18.0] * 6 + [1.0 / 36.0] * 12
relax_rate = 1.25


def lattice_step(pops, wet):
    vel = jnp.asarray(VELOCITIES.T.astype(np.float32))
    weights = jnp.asarray(np.array(WEIGHTS, np.float32))
    rho = jnp.sum(pops, axis=0)
    moment = jnp.einsum("dq,qabz->dabz", vel, pops, precision=lax.Precision.HIGHEST)
    speed = moment / rho[None]
    usq = jnp.sum(speed * speed, axis=0)
    proj = jnp.einsum("dq,dabz->qabz", vel, speed, precision=lax.Precision.HIGHEST)
    feq = weights[:, None, None, None] * rho[None] * (1.0 + 3.0 * proj + 4.5 * proj * proj - 1.5 * usq[None])
    post = jnp.where(wet[None], pops + relax_rate * (feq - pops), pops)
    sizea, sizeb = pops.shape[1], pops.shape[2]
    here = wet[1:-1, 1:-1]
    result = []
    for q in range(19):
        cx, cy, cz = int(VELOCITIES[q, 0]), int(VELOCITIES[q, 1]), int(VELOCITIES[q, 2])
        source = jnp.roll(post[q, 1 - cx:sizea - 1 - cx, 1 - cy:sizeb - 1 - cy], cz, axis=-1)
        source_wet = jnp.roll(wet[1 - cx:sizea - 1 - cx, 1 - cy:sizeb - 1 - cy], cz, axis=-1)
        bounced = post[OPPOSITE[q], 1:-1, 1:-1]
        result.append(jnp.where(here, jnp.where(source_wet, source, bounced), post[q, 1:-1, 1:-1]))
    return jnp.stack(result)


def reference(populations, fluid):
    wet = fluid == 1
    current = populations
    for step in range(STEPS):
        padded = jnp.pad(current, ((0, 0), (1, 1), (0, 0), (0, 0)), mode="wrap")
        padded = jnp.pad(padded, ((0, 0), (0, 0), (1, 1), (0, 0)))
        wet_pad = jnp.pad(wet, ((1, 1), (0, 0), (0, 0)), mode="wrap")
        wet_pad = jnp.pad(wet_pad, ((0, 0), (1, 1), (0, 0)))
        current = lattice_step(padded, wet_pad)
    return current
```

```python
import functools

import jax
import jax.numpy as jnp
import numpy as np
from jax import lax
from jax.experimental import pallas as pl
from jax.experimental.pallas import tpu as pltpu
from jax.sharding import PartitionSpec as P

STEPS = 4
DEPTH = 2
PAD = 8
RELAX = 1.25

VEL = [
    (0, 0, 0), (0, 0, 1), (0, 0, -1),
    (0, -1, 0), (0, -1, 1), (0, -1, -1),
    (0, 1, 0), (0, 1, 1), (0, 1, -1),
    (1, 1, 0), (1, 0, 0), (1, 0, 1), (1, 0, -1), (1, -1, 0),
    (-1, -1, 0), (-1, 0, 0), (-1, 0, 1), (-1, 0, -1), (-1, 1, 0),
]
REFERENCE_VEL = [
    (0, 0, 0), (1, 0, 0), (-1, 0, 0), (0, 1, 0), (0, -1, 0), (0, 0, 1), (0, 0, -1),
    (1, 1, 0), (-1, -1, 0), (1, -1, 0), (-1, 1, 0), (1, 0, 1), (-1, 0, -1),
    (1, 0, -1), (-1, 0, 1), (0, 1, 1), (0, -1, -1), (0, 1, -1), (0, -1, 1),
]
TO_REF = [REFERENCE_VEL.index(v) for v in VEL]
OPP = [VEL.index((-x, -y, -z)) for x, y, z in VEL]
WEIGHT = [(1.0 / 3.0, 1.0 / 18.0, 1.0 / 36.0)[abs(x) + abs(y) + abs(z)] for x, y, z in VEL]
DIRECTIONS = [(1, 0), (-1, 0), (0, 1), (0, -1), (1, 1), (1, -1), (-1, 1), (-1, -1)]


def runs(dx, dy):
    picks = [q for q in range(19) if (not dx or VEL[q][0] == dx) and (not dy or VEL[q][1] == dy)]
    result = []
    for q in picks:
        if result and result[-1][1] == q:
            result[-1][1] = q + 1
        else:
            result.append([q, q + 1])
    return result


def spans(d, offset, length, depth):
    if d == 0:
        return [(offset, offset, length, False)]
    inner = depth - 1
    if d > 0:
        full = (offset + length - inner, offset - inner, inner, False)
        edge = (offset + length - depth, offset - depth, 1, True)
    else:
        full = (offset, offset + length, inner, False)
        edge = (offset + inner, offset + length + inner, 1, True)
    return [full, edge] if inner else [edge]


def pieces(dx, dy, sizes, depth):
    lx, ly = sizes
    result = []
    for xs, xt, xn, xedge in spans(dx, depth, lx, depth):
        for ys, yt, yn, yedge in spans(dy, PAD, ly, depth):
            for lo, hi in runs(dx if xedge else 0, dy if yedge else 0):
                result.append((lo, hi - lo, xs, xt, xn, ys, yt, yn))
    return result


def mark_piece(dx, dy, sizes, depth):
    def along(d, offset, length):
        if d == 0:
            return offset, offset, length
        if d > 0:
            return offset + length - depth, offset - depth, depth
        return offset, offset + length, depth

    return along(dx, depth, sizes[0]) + along(dy, PAD, sizes[1])


def collide(f):
    pairs = [(q, OPP[q]) for q in range(1, 19) if q < OPP[q]]
    rho = f[0]
    moment = [None, None, None]
    for i, j in pairs:
        rho = rho + (f[i] + f[j])
        diff = f[i] - f[j]
        for axis in range(3):
            c = VEL[i][axis]
            if c:
                term = moment[axis]
                if term is None:
                    moment[axis] = diff if c > 0 else -diff
                else:
                    moment[axis] = term + diff if c > 0 else term - diff
    inverse = 1.0 / rho
    u = [m * inverse for m in moment]
    base = 1.0 - 1.5 * (u[0] * u[0] + u[1] * u[1] + u[2] * u[2])
    scaled = {w: (RELAX * w) * rho for w in set(WEIGHT)}
    keep = 1.0 - RELAX
    post = [None] * 19
    post[0] = keep * f[0] + scaled[WEIGHT[0]] * base
    for i, j in pairs:
        proj = None
        for axis in range(3):
            c = VEL[i][axis]
            if c:
                if proj is None:
                    proj = u[axis] if c > 0 else -u[axis]
                else:
                    proj = proj + u[axis] if c > 0 else proj - u[axis]
        even = scaled[WEIGHT[i]] * (base + 4.5 * (proj * proj))
        odd = scaled[WEIGHT[i]] * (3.0 * proj)
        post[i] = keep * f[i] + (even + odd)
        post[j] = keep * f[j] + (even - odd)
    return post


def row_starts(ring, ly):
    first, last = PAD - ring, PAD + ly + ring
    starts = list(range(first, last - 7, 8))
    if starts[-1] + 8 < last:
        starts.append(last - 8)
    return starts


def stream(buf, marks, layer, row):
    result = []
    for q, (cx, cy, cz) in enumerate(VEL):
        if q == 0:
            result.append(buf[0, layer, pl.ds(row, 8), :])
            continue
        source = buf[q, layer - cx, pl.ds(row - cy, 8), :]
        if cz:
            source = pltpu.roll(source, cz % source.shape[-1], 1)
        open_ = marks[cz % 3, layer - cx, pl.ds(row - cy, 8), :] != 0
        result.append(jnp.where(open_, source, buf[OPP[q], layer, pl.ds(row, 8), :]))
    return result


def kernel(axes, sizes, depth, pops_hbm, fluid_hbm, out_hbm, first, last_f, marks, *rest):
    rounds = STEPS // depth
    bufs, rest = rest[:rounds], rest[rounds:]
    inner, rest = rest[: depth - 1], rest[depth - 1 :]
    in_sem, out_sem, mark_send, mark_recv, send_sem, recv_sem = rest
    lx, ly = sizes
    nx, ny = axes
    ix, iy = lax.axis_index("gx"), lax.axis_index("gy")
    has = {0: None, 1: iy < ny - 1, -1: iy > 0}

    def when(condition, action):
        if condition is None:
            action()
        else:
            pl.when(condition)(action)

    def target(dx, dy):
        return {"gx": lax.rem(ix + nx + dx, nx), "gy": iy + dy}

    fluid_in = pltpu.make_async_copy(
        fluid_hbm, marks.at[0, pl.ds(depth, lx), pl.ds(PAD, ly)], in_sem.at[lx]
    )
    fluid_in.start()
    loads = [
        pltpu.make_async_copy(pops_hbm.at[:, a], first.at[:, a], in_sem.at[a]) for a in range(lx)
    ]
    for load in loads:
        load.start()

    barrier = pltpu.get_barrier_semaphore()
    for dx, dy in DIRECTIONS:
        when(
            has[dy],
            lambda dx=dx, dy=dy: pl.semaphore_signal(
                barrier, inc=1, device_id=target(dx, dy), device_id_type=pl.DeviceIdType.MESH
            ),
        )

    for edge, rows in ((iy == 0, PAD - depth), (iy == ny - 1, PAD + ly)):

        @pl.when(edge)
        def _():
            for a in range(lx + 2 * depth):
                marks[0, a, rows : rows + depth, :] = jnp.zeros((depth, marks.shape[-1]), jnp.int32)

    def post_layer(a):
        f = [first[TO_REF[q], a] for q in range(19)]
        for q, value in enumerate(collide(f)):
            bufs[0][q, depth + a, PAD : PAD + ly, :] = value

    order = sorted(range(lx), key=lambda a: min(a, lx - 1 - a))
    for a in order:
        loads[a].wait()
        post_layer(a)
    fluid_in.wait()

    peers = 2 + 3 * (iy > 0).astype(jnp.int32) + 3 * (iy < ny - 1).astype(jnp.int32)
    pl.semaphore_wait(barrier, peers)

    def exchange(copies):
        for (dx, dy), group in copies:
            when(has[dy], lambda group=group: [c.start() for c in group] and None)

    def arrive(copies):
        for (dx, dy), group in copies:
            when(has[-dy], lambda group=group: [c.wait_recv() for c in group] and None)

    def drain(copies):
        for (dx, dy), group in copies:
            when(has[dy], lambda group=group: [c.wait_send() for c in group] and None)

    def mark_copies():
        result = []
        for i, (dx, dy) in enumerate(DIRECTIONS):
            xs, xt, xn, ys, yt, yn = mark_piece(dx, dy, sizes, depth)
            result.append(
                (
                    (dx, dy),
                    [
                        pltpu.make_async_remote_copy(
                            src_ref=marks.at[0, pl.ds(xs, xn), pl.ds(ys, yn)],
                            dst_ref=marks.at[0, pl.ds(xt, xn), pl.ds(yt, yn)],
                            send_sem=mark_send.at[i],
                            recv_sem=mark_recv.at[i],
                            device_id=target(dx, dy),
                            device_id_type=pl.DeviceIdType.MESH,
                        )
                    ],
                )
            )
        return result

    def halo_copies(turn):
        buf = bufs[turn]
        result, count = [], 0
        for dx, dy in DIRECTIONS:
            group = []
            for lo, n, xs, xt, xn, ys, yt, yn in pieces(dx, dy, sizes, depth):
                group.append(
                    pltpu.make_async_remote_copy(
                        src_ref=buf.at[pl.ds(lo, n), pl.ds(xs, xn), pl.ds(ys, yn)],
                        dst_ref=buf.at[pl.ds(lo, n), pl.ds(xt, xn), pl.ds(yt, yn)],
                        send_sem=send_sem.at[turn, count],
                        recv_sem=recv_sem.at[turn, count],
                        device_id=target(dx, dy),
                        device_id_type=pl.DeviceIdType.MESH,
                    )
                )
                count += 1
            result.append(((dx, dy), group))
        return result

    mark_list = mark_copies()
    exchange(mark_list)
    halos = [halo_copies(turn) for turn in range(rounds)]
    exchange(halos[0])

    arrive(mark_list)
    for a in range(lx + 2 * depth):
        for row in row_starts(depth, ly):
            here = marks[0, a, row : row + 8, :]
            lanes = here.shape[-1]
            marks[1, a, row : row + 8, :] = pltpu.roll(here, 1, 1)
            marks[2, a, row : row + 8, :] = pltpu.roll(here, lanes - 1, 1)

    stores = []
    for turn in range(rounds):
        arrive(halos[turn])
        source = bufs[turn]
        for ring in range(depth - 1, -1, -1):
            final = turn == rounds - 1 and ring == 0
            for a in range(-ring, lx + ring):
                for row in row_starts(ring, ly):
                    f = stream(source, marks, depth + a, row)
                    if final:
                        wet = marks[0, depth + a, row : row + 8, :] != 0
                        for q in range(19):
                            old = first[TO_REF[q], a, row - PAD : row - PAD + 8, :]
                            last_f[TO_REF[q], a, row - PAD : row - PAD + 8, :] = jnp.where(
                                wet, f[q], old
                            )
                    else:
                        into = inner[ring - 1] if ring else bufs[turn + 1]
                        for q, value in enumerate(collide(f)):
                            into[q, depth + a, row : row + 8, :] = value
                if final:
                    store = pltpu.make_async_copy(last_f.at[:, a], out_hbm.at[:, a], out_sem.at[a])
                    store.start()
                    stores.append(store)
            if ring:
                source = inner[ring - 1]
        if turn + 1 < rounds:
            exchange(halos[turn + 1])
    drain(mark_list)
    for turn in range(rounds):
        drain(halos[turn])
    for store in stores:
        store.wait()


def per_device(axes, depth, populations, fluid):
    sizes = fluid.shape[:2]
    lx, ly = sizes
    nz = fluid.shape[2]
    rounds = STEPS // depth
    wide = (lx + 2 * depth, ly + 2 * PAD, nz)
    count = sum(len(pieces(dx, dy, sizes, depth)) for dx, dy in DIRECTIONS)
    dma = pltpu.SemaphoreType.DMA
    return pl.pallas_call(
        functools.partial(kernel, axes, sizes, depth),
        out_shape=jax.ShapeDtypeStruct(populations.shape, populations.dtype),
        in_specs=[pl.BlockSpec(memory_space=pl.ANY)] * 2,
        out_specs=pl.BlockSpec(memory_space=pl.ANY),
        scratch_shapes=[
            pltpu.VMEM(populations.shape, jnp.float32),
            pltpu.VMEM(populations.shape, jnp.float32),
            pltpu.VMEM((3,) + wide, jnp.int32),
        ]
        + [pltpu.VMEM((19,) + wide, jnp.float32)] * (rounds + depth - 1)
        + [
            dma((lx + 1,)),
            dma((lx,)),
            dma((len(DIRECTIONS),)),
            dma((len(DIRECTIONS),)),
            dma((rounds, count)),
            dma((rounds, count)),
        ],
        compiler_params=pltpu.CompilerParams(collective_id=0, has_side_effects=True),
    )(populations, fluid)


def solution(mesh):
    axes = (mesh.shape["gx"], mesh.shape["gy"])
    return jax.shard_map(
        functools.partial(per_device, axes, DEPTH),
        mesh=mesh,
        in_specs=(P(None, "gx", "gy", None), P("gx", "gy", None)),
        out_specs=P(None, "gx", "gy", None),
        check_vma=False,
    )
```

```python
import functools

import jax
import jax.numpy as jnp
import numpy as np
from jax import lax
from jax.experimental import pallas as pl
from jax.experimental.pallas import tpu as pltpu
from jax.sharding import PartitionSpec as P

STEPS = 4
DEPTH = 4
PAD = 8
RELAX = 1.25

VEL = [
    (0, 0, 0), (0, 0, 1), (0, 0, -1),
    (0, -1, 0), (0, -1, 1), (0, -1, -1),
    (0, 1, 0), (0, 1, 1), (0, 1, -1),
    (1, 1, 0), (1, 0, 0), (1, 0, 1), (1, 0, -1), (1, -1, 0),
    (-1, -1, 0), (-1, 0, 0), (-1, 0, 1), (-1, 0, -1), (-1, 1, 0),
]
REFERENCE_VEL = [
    (0, 0, 0), (1, 0, 0), (-1, 0, 0), (0, 1, 0), (0, -1, 0), (0, 0, 1), (0, 0, -1),
    (1, 1, 0), (-1, -1, 0), (1, -1, 0), (-1, 1, 0), (1, 0, 1), (-1, 0, -1),
    (1, 0, -1), (-1, 0, 1), (0, 1, 1), (0, -1, -1), (0, 1, -1), (0, -1, 1),
]
TO_REF = [REFERENCE_VEL.index(v) for v in VEL]
OPP = [VEL.index((-x, -y, -z)) for x, y, z in VEL]
WEIGHT = [(1.0 / 3.0, 1.0 / 18.0, 1.0 / 36.0)[abs(x) + abs(y) + abs(z)] for x, y, z in VEL]
DIRECTIONS = [(1, 0), (-1, 0), (0, 1), (0, -1), (1, 1), (1, -1), (-1, 1), (-1, -1)]


def runs(dx, dy):
    picks = [q for q in range(19) if (not dx or VEL[q][0] == dx) and (not dy or VEL[q][1] == dy)]
    result = []
    for q in picks:
        if result and result[-1][1] == q:
            result[-1][1] = q + 1
        else:
            result.append([q, q + 1])
    return result


def spans(d, offset, length, depth):
    if d == 0:
        return [(offset, offset, length, False)]
    inner = depth - 1
    if d > 0:
        full = (offset + length - inner, offset - inner, inner, False)
        edge = (offset + length - depth, offset - depth, 1, True)
    else:
        full = (offset, offset + length, inner, False)
        edge = (offset + inner, offset + length + inner, 1, True)
    return [full, edge] if inner else [edge]


def pieces(dx, dy, sizes, depth):
    lx, ly = sizes
    result = []
    for xs, xt, xn, xedge in spans(dx, depth, lx, depth):
        for ys, yt, yn, yedge in spans(dy, PAD, ly, depth):
            for lo, hi in runs(dx if xedge else 0, dy if yedge else 0):
                result.append((lo, hi - lo, xs, xt, xn, ys, yt, yn))
    return result


def mark_piece(dx, dy, sizes, depth):
    def along(d, offset, length):
        if d == 0:
            return offset, offset, length
        if d > 0:
            return offset + length - depth, offset - depth, depth
        return offset, offset + length, depth

    return along(dx, depth, sizes[0]) + along(dy, PAD, sizes[1])


def collide(f):
    pairs = [(q, OPP[q]) for q in range(1, 19) if q < OPP[q]]
    rho = f[0]
    moment = [None, None, None]
    for i, j in pairs:
        rho = rho + (f[i] + f[j])
        diff = f[i] - f[j]
        for axis in range(3):
            c = VEL[i][axis]
            if c:
                term = moment[axis]
                if term is None:
                    moment[axis] = diff if c > 0 else -diff
                else:
                    moment[axis] = term + diff if c > 0 else term - diff
    inverse = 1.0 / rho
    u = [m * inverse for m in moment]
    base = 1.0 - 1.5 * (u[0] * u[0] + u[1] * u[1] + u[2] * u[2])
    scaled = {w: (RELAX * w) * rho for w in set(WEIGHT)}
    keep = 1.0 - RELAX
    post = [None] * 19
    post[0] = keep * f[0] + scaled[WEIGHT[0]] * base
    for i, j in pairs:
        proj = None
        for axis in range(3):
            c = VEL[i][axis]
            if c:
                if proj is None:
                    proj = u[axis] if c > 0 else -u[axis]
                else:
                    proj = proj + u[axis] if c > 0 else proj - u[axis]
        even = scaled[WEIGHT[i]] * (base + 4.5 * (proj * proj))
        odd = scaled[WEIGHT[i]] * (3.0 * proj)
        post[i] = keep * f[i] + (even + odd)
        post[j] = keep * f[j] + (even - odd)
    return post


def row_starts(ring, ly):
    first, last = PAD - ring, PAD + ly + ring
    starts = list(range(first, last - 7, 8))
    if starts[-1] + 8 < last:
        starts.append(last - 8)
    return starts


def stream(buf, marks, layer, row):
    result = []
    for q, (cx, cy, cz) in enumerate(VEL):
        if q == 0:
            result.append(buf[0, layer, pl.ds(row, 8), :])
            continue
        source = buf[q, layer - cx, pl.ds(row - cy, 8), :]
        if cz:
            source = pltpu.roll(source, cz % source.shape[-1], 1)
        open_ = marks[cz % 3, layer - cx, pl.ds(row - cy, 8), :] != 0
        result.append(jnp.where(open_, source, buf[OPP[q], layer, pl.ds(row, 8), :]))
    return result


def kernel(axes, sizes, depth, pops_hbm, fluid_hbm, out_hbm, first, last_f, marks, *rest):
    rounds = STEPS // depth
    bufs, rest = rest[:rounds], rest[rounds:]
    inner, rest = rest[: depth - 1], rest[depth - 1 :]
    in_sem, out_sem, mark_send, mark_recv, send_sem, recv_sem = rest
    lx, ly = sizes
    nx, ny = axes
    ix, iy = lax.axis_index("gx"), lax.axis_index("gy")
    has = {0: None, 1: iy < ny - 1, -1: iy > 0}

    def when(condition, action):
        if condition is None:
            action()
        else:
            pl.when(condition)(action)

    def target(dx, dy):
        return {"gx": lax.rem(ix + nx + dx, nx), "gy": iy + dy}

    fluid_in = pltpu.make_async_copy(
        fluid_hbm, marks.at[0, pl.ds(depth, lx), pl.ds(PAD, ly)], in_sem.at[lx]
    )
    loads = [
        pltpu.make_async_copy(pops_hbm.at[:, a], first.at[:, a], in_sem.at[a]) for a in range(lx)
    ]

    barrier = pltpu.get_barrier_semaphore()
    for dx, dy in DIRECTIONS:
        when(
            has[dy],
            lambda dx=dx, dy=dy: pl.semaphore_signal(
                barrier, inc=1, device_id=target(dx, dy), device_id_type=pl.DeviceIdType.MESH
            ),
        )

    fluid_in.start()
    for load in loads:
        load.start()

    for edge, rows in ((iy == 0, PAD - depth), (iy == ny - 1, PAD + ly)):

        @pl.when(edge)
        def _():
            for a in range(lx + 2 * depth):
                marks[0, a, rows : rows + depth, :] = jnp.zeros((depth, marks.shape[-1]), jnp.int32)

    def post_layer(a):
        f = [first[TO_REF[q], a] for q in range(19)]
        for q, value in enumerate(collide(f)):
            bufs[0][q, depth + a, PAD : PAD + ly, :] = value

    order = sorted(range(lx), key=lambda a: min(a, lx - 1 - a))
    for a in order:
        loads[a].wait()
        post_layer(a)
    fluid_in.wait()

    peers = 2 + 3 * (iy > 0).astype(jnp.int32) + 3 * (iy < ny - 1).astype(jnp.int32)
    pl.semaphore_wait(barrier, peers)

    def exchange(copies):
        for (dx, dy), group in copies:
            when(has[dy], lambda group=group: [c.start() for c in group] and None)

    def arrive(copies):
        for (dx, dy), group in copies:
            when(has[-dy], lambda group=group: [c.wait_recv() for c in group] and None)

    def drain(copies):
        for (dx, dy), group in copies:
            when(has[dy], lambda group=group: [c.wait_send() for c in group] and None)

    def mark_copies():
        result = []
        for i, (dx, dy) in enumerate(DIRECTIONS):
            xs, xt, xn, ys, yt, yn = mark_piece(dx, dy, sizes, depth)
            result.append(
                (
                    (dx, dy),
                    [
                        pltpu.make_async_remote_copy(
                            src_ref=marks.at[0, pl.ds(xs, xn), pl.ds(ys, yn)],
                            dst_ref=marks.at[0, pl.ds(xt, xn), pl.ds(yt, yn)],
                            send_sem=mark_send.at[i],
                            recv_sem=mark_recv.at[i],
                            device_id=target(dx, dy),
                            device_id_type=pl.DeviceIdType.MESH,
                        )
                    ],
                )
            )
        return result

    def halo_copies(turn):
        buf = bufs[turn]
        result, count = [], 0
        for dx, dy in DIRECTIONS:
            group = []
            for lo, n, xs, xt, xn, ys, yt, yn in pieces(dx, dy, sizes, depth):
                group.append(
                    pltpu.make_async_remote_copy(
                        src_ref=buf.at[pl.ds(lo, n), pl.ds(xs, xn), pl.ds(ys, yn)],
                        dst_ref=buf.at[pl.ds(lo, n), pl.ds(xt, xn), pl.ds(yt, yn)],
                        send_sem=send_sem.at[turn, count],
                        recv_sem=recv_sem.at[turn, count],
                        device_id=target(dx, dy),
                        device_id_type=pl.DeviceIdType.MESH,
                    )
                )
                count += 1
            result.append(((dx, dy), group))
        return result

    mark_list = mark_copies()
    exchange(mark_list)
    halos = [halo_copies(turn) for turn in range(rounds)]
    exchange(halos[0])

    arrive(mark_list)
    for a in range(lx + 2 * depth):
        for row in row_starts(depth, ly):
            here = marks[0, a, row : row + 8, :]
            lanes = here.shape[-1]
            marks[1, a, row : row + 8, :] = pltpu.roll(here, 1, 1)
            marks[2, a, row : row + 8, :] = pltpu.roll(here, lanes - 1, 1)

    stores = []
    for turn in range(rounds):
        arrive(halos[turn])
        source = bufs[turn]
        for ring in range(depth - 1, -1, -1):
            final = turn == rounds - 1 and ring == 0
            for a in range(-ring, lx + ring):
                for row in row_starts(ring, ly):
                    f = stream(source, marks, depth + a, row)
                    if final:
                        wet = marks[0, depth + a, row : row + 8, :] != 0
                        for q in range(19):
                            old = first[TO_REF[q], a, row - PAD : row - PAD + 8, :]
                            last_f[TO_REF[q], a, row - PAD : row - PAD + 8, :] = jnp.where(
                                wet, f[q], old
                            )
                    else:
                        into = inner[ring - 1] if ring else bufs[turn + 1]
                        for q, value in enumerate(collide(f)):
                            into[q, depth + a, row : row + 8, :] = value
                if final:
                    store = pltpu.make_async_copy(last_f.at[:, a], out_hbm.at[:, a], out_sem.at[a])
                    store.start()
                    stores.append(store)
            if ring:
                source = inner[ring - 1]
        if turn + 1 < rounds:
            exchange(halos[turn + 1])
    drain(mark_list)
    for turn in range(rounds):
        drain(halos[turn])
    for store in stores:
        store.wait()


def per_device(axes, depth, populations, fluid):
    sizes = fluid.shape[:2]
    lx, ly = sizes
    nz = fluid.shape[2]
    rounds = STEPS // depth
    wide = (lx + 2 * depth, ly + 2 * PAD, nz)
    count = sum(len(pieces(dx, dy, sizes, depth)) for dx, dy in DIRECTIONS)
    dma = pltpu.SemaphoreType.DMA
    return pl.pallas_call(
        functools.partial(kernel, axes, sizes, depth),
        out_shape=jax.ShapeDtypeStruct(populations.shape, populations.dtype),
        in_specs=[pl.BlockSpec(memory_space=pl.ANY)] * 2,
        out_specs=pl.BlockSpec(memory_space=pl.ANY),
        scratch_shapes=[
            pltpu.VMEM(populations.shape, jnp.float32),
            pltpu.VMEM(populations.shape, jnp.float32),
            pltpu.VMEM((3,) + wide, jnp.int32),
        ]
        + [pltpu.VMEM((19,) + wide, jnp.float32)] * (rounds + depth - 1)
        + [
            dma((lx + 1,)),
            dma((lx,)),
            dma((len(DIRECTIONS),)),
            dma((len(DIRECTIONS),)),
            dma((rounds, count)),
            dma((rounds, count)),
        ],
        compiler_params=pltpu.CompilerParams(collective_id=0, has_side_effects=True),
    )(populations, fluid)


def solution(mesh):
    axes = (mesh.shape["gx"], mesh.shape["gy"])
    return jax.shard_map(
        functools.partial(per_device, axes, DEPTH),
        mesh=mesh,
        in_specs=(P(None, "gx", "gy", None), P("gx", "gy", None)),
        out_specs=P(None, "gx", "gy", None),
        check_vma=False,
    )
```
